16 devices in a mesh: ep: 16 (over z, y, x, core).
Axes of the slice: x: 2, y: 2, z: 2, core: 2. Of those that a mesh axis runs over, the one named last changes fastest.
Arguments:
- hidden: bfloat16 [2048, 4096], P('ep')
- grad_out: bfloat16 [2048, 4096], P('ep')
- w_router: bfloat16 [4096, 16], replicated
- b_router: float32 [16], replicated
- expert_ids: int32 [2048, 4], P('ep')
- slot_ids: int32 [2048, 4], P('ep')
- w_gate_up: bfloat16 [16, 4096, 1376], P('ep')
- b_gate_up: float32 [16, 1376], P('ep')
- w_down: bfloat16 [16, 688, 4096], P('ep')
- b_down: float32 [16, 4096], P('ep')
Outputs:
- output 1: bfloat16 [2048, 4096], P('ep')
- output 2: bfloat16 [2048, 4096], P('ep')
- output 3: float32 [4096, 16], replicated
- output 4: float32 [16], replicated
- output 5: float32 [16, 4096, 1376], P('ep')
- output 6: float32 [16, 1376], P('ep')
- output 7: float32 [16, 688, 4096], P('ep')
- output 8: float32 [16, 4096], P('ep')
All inputs are finite; a program needn't handle non-finite values.
Results may differ from the reference program's by a relative error of at most 0.0100469.
Values are sent between devices in bfloat16 or wider.
A program may use at most 1 GiB of HBM per device.

```python
import jax
import jax.numpy as jnp
from jax import lax

D_MODEL = 4096
FF_EXPERT = 688
EXPERTS = 16
TOP_K = 4
TOKENS_DEV = 128
EP_DEVICES = 16

TOKENS = EP_DEVICES * TOKENS_DEV
CAPACITY = (3 * TOKENS_DEV * TOP_K + 2 * EXPERTS - 1) // (2 * EXPERTS)
ROWS_EXPERT = EP_DEVICES * CAPACITY
SWIGLU_LIMIT = 7.0
SWIGLU_ALPHA = 1.702


def draw_routing(key):
    key_bias, key_dev = jax.random.split(key)
    expert_bias = jax.random.randint(key_bias, (EXPERTS,), 0, 512)
    expert_range = jnp.arange(EXPERTS, dtype=jnp.int32)
    copies = TOKENS_DEV * TOP_K

    def one_device(dev_key):
        key_noise, key_hot, key_pick, key_prio = jax.random.split(dev_key, 4)
        noise_int = jax.random.randint(key_noise, (TOKENS_DEV, EXPERTS), 0, 1024)
        hot_expert = jax.random.randint(key_hot, (), 0, EXPERTS)
        forced = jax.random.permutation(key_pick, TOKENS_DEV) < 2 * CAPACITY
        hot_bonus = jnp.where(forced[:, None] & (expert_range[None, :] == hot_expert), 4096, 0)
        scores = (noise_int + expert_bias[None, :] + hot_bonus) * EXPERTS + expert_range[None, :]
        choice = lax.top_k(scores, TOP_K)[1].astype(jnp.int32)
        flat_ids = choice.reshape(-1)
        priority = jax.random.permutation(key_prio, copies)
        sort_order = jnp.argsort(flat_ids * copies + priority)
        counts = jnp.bincount(flat_ids, length=EXPERTS)
        starts = jnp.cumsum(counts) - counts
        rank_sorted = (jnp.arange(copies, dtype=jnp.int32) - starts[flat_ids[sort_order]]).astype(jnp.int32)
        slot_rank = jnp.zeros((copies,), jnp.int32).at[sort_order].set(rank_sorted)
        slot_ids = jnp.where(slot_rank < CAPACITY, slot_rank, -1).reshape(TOKENS_DEV, TOP_K)
        return choice, slot_ids

    choice, slot_ids = jax.vmap(one_device)(jax.random.split(key_dev, EP_DEVICES))
    return choice.reshape(TOKENS, TOP_K), slot_ids.reshape(TOKENS, TOP_K).astype(jnp.int32)


def setup_inputs(seed: int = 0) -> dict:
    key_list = jax.random.split(jax.random.key(seed), 9)
    hidden = jax.random.normal(key_list[0], (TOKENS, D_MODEL), jnp.float32).astype(jnp.bfloat16)
    grad_out = jax.random.normal(key_list[1], (TOKENS, D_MODEL), jnp.float32).astype(jnp.bfloat16)
    w_router = (2.0 * D_MODEL ** -0.5 * jax.random.normal(key_list[2], (D_MODEL, EXPERTS), jnp.float32)).astype(jnp.bfloat16)
    b_router = jax.random.normal(key_list[3], (EXPERTS,), jnp.float32)
    expert_ids, slot_ids = draw_routing(key_list[4])
    w_gate_up = (3.0 * D_MODEL ** -0.5 * jax.random.normal(key_list[5], (EXPERTS, D_MODEL, 2 * FF_EXPERT), jnp.float32)).astype(jnp.bfloat16)
    b_gate_up = jax.random.normal(key_list[6], (EXPERTS, 2 * FF_EXPERT), jnp.float32)
    w_down = (0.15 * FF_EXPERT ** -0.5 * jax.random.normal(key_list[7], (EXPERTS, FF_EXPERT, D_MODEL), jnp.float32)).astype(jnp.bfloat16)
    b_down = 0.5 * jax.random.normal(key_list[8], (EXPERTS, D_MODEL), jnp.float32)
    return {'hidden': hidden, 'grad_out': grad_out, 'w_router': w_router, 'b_router': b_router, 'expert_ids': expert_ids, 'slot_ids': slot_ids, 'w_gate_up': w_gate_up, 'b_gate_up': b_gate_up, 'w_down': w_down, 'b_down': b_down}


def swiglu(pre_act):
    col_pairs = pre_act.reshape(pre_act.shape[:-1] + (pre_act.shape[-1] // 2, 2))
    gate_in = jnp.minimum(col_pairs[..., 0], SWIGLU_LIMIT)
    up_in = jnp.clip(col_pairs[..., 1], -SWIGLU_LIMIT, SWIGLU_LIMIT)
    return gate_in * jax.nn.sigmoid(SWIGLU_ALPHA * gate_in) * (up_in + 1.0)


def reference(hidden, grad_out, w_router, b_router, expert_ids, slot_ids, w_gate_up, b_gate_up, w_down, b_down):
    buf_total = EXPERTS * ROWS_EXPERT
    copy_count = TOKENS * TOP_K
    src_dev = (jnp.arange(TOKENS, dtype=jnp.int32) // TOKENS_DEV)[:, None]
    dest_row = jnp.where(slot_ids >= 0, expert_ids * ROWS_EXPERT + src_dev * CAPACITY + slot_ids, buf_total)
    src_copy = jnp.full((buf_total + 1,), copy_count, jnp.int32).at[dest_row.reshape(-1)].set(jnp.arange(copy_count, dtype=jnp.int32))[:buf_total].reshape(EXPERTS, ROWS_EXPERT)
    logits = jnp.dot(hidden, w_router, preferred_element_type=jnp.float32) + b_router
    gate_w = jax.nn.softmax(jnp.take_along_axis(logits, expert_ids, axis=1), axis=-1)
    flat_gate = gate_w.reshape(-1)

    def expert_forward(expert_args):
        w_gu, b_gu, w_dn, b_dn, src_rows = expert_args
        x_rows = jnp.take(hidden, src_rows // TOP_K, axis=0, mode='fill', fill_value=0)
        pre_act = jnp.dot(x_rows, w_gu, preferred_element_type=jnp.float32) + b_gu
        act_bf = swiglu(pre_act).astype(jnp.bfloat16)
        return (jnp.dot(act_bf, w_dn, preferred_element_type=jnp.float32) + b_dn).astype(jnp.bfloat16)

    y_flat = lax.map(expert_forward, (w_gate_up, b_gate_up, w_down, b_down, src_copy)).reshape(buf_total, D_MODEL)

    def token_forward(block_args):
        gate_blk, dest_blk, grad_blk = block_args
        y_blk = jnp.take(y_flat, dest_blk, axis=0, mode='fill', fill_value=0).astype(jnp.float32)
        out_blk = jnp.sum(gate_blk[:, :, None] * y_blk, axis=1).astype(jnp.bfloat16)
        return out_blk, jnp.einsum('td,tkd->tk', grad_blk.astype(jnp.float32), y_blk)

    dev_shape = (EP_DEVICES, TOKENS_DEV)
    block_out, gate_grad = lax.map(token_forward, (gate_w.reshape(dev_shape + (TOP_K,)), dest_row.reshape(dev_shape + (TOP_K,)), grad_out.reshape(dev_shape + (D_MODEL,))))
    block_out = block_out.reshape(TOKENS, D_MODEL)
    gate_grad = gate_grad.reshape(TOKENS, TOP_K)
    sel_grad = gate_w * (gate_grad - jnp.sum(gate_w * gate_grad, axis=1, keepdims=True))
    logit_grad = jnp.zeros((TOKENS, EXPERTS), jnp.float32).at[jnp.arange(TOKENS)[:, None], expert_ids].add(sel_grad).astype(jnp.bfloat16)

    def expert_backward(expert_args):
        w_gu, b_gu, w_dn, src_rows = expert_args
        tok_rows = src_rows // TOP_K
        x_rows = jnp.take(hidden, tok_rows, axis=0, mode='fill', fill_value=0)
        pre_act = jnp.dot(x_rows, w_gu, preferred_element_type=jnp.float32) + b_gu
        act_val, act_vjp = jax.vjp(swiglu, pre_act)
        act_bf = act_val.astype(jnp.bfloat16)
        row_gate = jnp.take(flat_gate, src_rows, axis=0, mode='fill', fill_value=0)
        row_grad = jnp.take(grad_out, tok_rows, axis=0, mode='fill', fill_value=0).astype(jnp.float32)
        q_rows = (row_gate[:, None] * row_grad).astype(jnp.bfloat16)
        grad_b_dn = jnp.sum(q_rows.astype(jnp.float32), axis=0)
        grad_w_dn = jnp.dot(act_bf.T, q_rows, preferred_element_type=jnp.float32)
        act_grad = jnp.dot(q_rows, w_dn.T, preferred_element_type=jnp.float32)
        pre_grad = act_vjp(act_grad)[0].astype(jnp.bfloat16)
        grad_b_gu = jnp.sum(pre_grad.astype(jnp.float32), axis=0)
        grad_w_gu = jnp.dot(x_rows.T, pre_grad, preferred_element_type=jnp.float32)
        p_rows = jnp.dot(pre_grad, w_gu.T, preferred_element_type=jnp.float32).astype(jnp.bfloat16)
        return grad_w_gu, grad_b_gu, grad_w_dn, grad_b_dn, p_rows

    grad_w_gate_up, grad_b_gate_up, grad_w_down, grad_b_down, p_rows = lax.map(expert_backward, (w_gate_up, b_gate_up, w_down, src_copy))
    p_flat = p_rows.reshape(buf_total, D_MODEL)

    def token_backward(block_args):
        dest_blk, logit_blk = block_args
        p_blk = jnp.take(p_flat, dest_blk, axis=0, mode='fill', fill_value=0).astype(jnp.float32)
        router_dx = jnp.dot(logit_blk, w_router.T, preferred_element_type=jnp.float32)
        return (jnp.sum(p_blk, axis=1) + router_dx).astype(jnp.bfloat16)

    grad_hidden = lax.map(token_backward, (dest_row.reshape(dev_shape + (TOP_K,)), logit_grad.reshape(dev_shape + (EXPERTS,)))).reshape(TOKENS, D_MODEL)
    grad_w_router = jnp.dot(hidden.T, logit_grad, preferred_element_type=jnp.float32)
    grad_b_router = jnp.sum(logit_grad.astype(jnp.float32), axis=0)
    return (block_out, grad_hidden, grad_w_router, grad_b_router, grad_w_gate_up, grad_b_gate_up, grad_w_down, grad_b_down)
```

```python
import functools

import jax
import jax.numpy as jnp
from jax import lax
from jax.experimental import pallas as pl
from jax.experimental.pallas import tpu as pltpu
from jax.sharding import PartitionSpec as P

SWIGLU_LIMIT = 7.0
SWIGLU_ALPHA = 1.702
MESH_ID = pl.DeviceIdType.MESH
BF = jnp.bfloat16
F32 = jnp.float32

DIMS = (2, 4, 8)
CHIP_ORDER = (3, 4, 5, 2, 6, 1, 7)
NDEV = 16


def flip(me, mask):
    out = 0
    for b in (1, 2, 4, 8):
        bit = lax.rem(lax.div(me, b), 2)
        if isinstance(mask, int):
            if mask & b:
                bit = 1 - bit
        else:
            bit = lax.rem(bit + lax.rem(lax.div(mask, b), 2), 2)
        out = out + b * bit
    return out


def split3(v):
    hi = v.astype(BF)
    rest = v - hi.astype(F32)
    mid = rest.astype(BF)
    low = (rest - mid.astype(F32)).astype(BF)
    return hi, mid, low


def dot(a, b):
    return jnp.dot(a, b, preferred_element_type=F32)


def dot_nt(a, b):
    return lax.dot_general(a, b, (((1,), (1,)), ((), ())), preferred_element_type=F32)


def remote(src, dst, ssem, rsem, dev):
    return pltpu.make_async_remote_copy(src_ref=src, dst_ref=dst, send_sem=ssem, recv_sem=rsem,
                                        device_id=(dev,), device_id_type=MESH_ID)


def block_kernel(cfg, *refs):
    T, D, F, C = cfg
    F2 = 2 * F
    R = NDEV * C
    NT = -(-F // 128)
    FP = NT * 128
    (x_ref, dy_ref, wr_ref, br_ref, eid_ref, sid_ref, wgu_ref, bgu_ref, wd_ref, bd_ref,
     out_ref, dx_ref, dwr_ref, dbr_ref, dbd_ref, dbgu_ref, rx_o, q_o, a_o, dh_o,
     xall, dyall, yret, pret,
     wgu, wd, rx, rq, gs, us, asc, dh, yv, pv, xs, xv, dyv, acc, meta, dlall, mcol, emat,
     ag_s, ag_r, co_s, co_r, ya_s, ya_r, pa_s, pa_r, me_s, me_r, dl_s, dl_r, loc, tile_sem) = refs
    me = lax.axis_index("ep")
    lane = lambda shape: lax.broadcasted_iota(jnp.int32, shape, 1)
    sub = lambda shape: lax.broadcasted_iota(jnp.int32, shape, 0)

    ld_x = pltpu.make_async_copy(x_ref, xv, loc.at[0]); ld_x.start()
    ld_dy = pltpu.make_async_copy(dy_ref, dyv, loc.at[1]); ld_dy.start()
    ld_gu = pltpu.make_async_copy(wgu_ref, wgu, loc.at[2]); ld_gu.start()
    ld_d = pltpu.make_async_copy(wd_ref, wd.at[pl.ds(0, F)], loc.at[3]); ld_d.start()

    bar = pltpu.get_barrier_semaphore()
    for m in range(1, NDEV):
        pl.semaphore_signal(bar, inc=1, device_id=(flip(me, m),), device_id_type=MESH_ID)
    pl.semaphore_wait(bar, NDEV - 1)

    cuts = [0, 11 * D // 32, 22 * D // 32, D]
    srcs, alls = (x_ref, dy_ref), (xall, dyall)

    def offs(j):
        a, b, c = DIMS[j], DIMS[(j + 1) % 3], DIMS[(j + 2) % 3]
        return (a, b, c), (a, b, b ^ a, c, c ^ a, c ^ b, c ^ a ^ b)

    def cols(j):
        return pl.ds(cuts[j], cuts[j + 1] - cuts[j])

    def ag_copy(w, j, stage, t):
        order, _ = offs(j)
        tgt = order[stage]
        off = (0, order[0], order[1], order[0] ^ order[1])[t]
        idx = (0, 1, 3)[stage] + t
        shard = flip(me, off)
        src = srcs[w].at[:, cols(j)] if off == 0 else alls[w].at[shard, :, cols(j)]
        return remote(src, alls[w].at[shard, :, cols(j)], ag_s.at[w, j, idx], ag_r.at[w, j, idx], flip(me, tgt))

    def co_copy(w, j, idx):
        _, off = offs(j)
        shard = flip(me, off[idx])
        return remote(alls[w].at[shard, :, cols(j)], alls[w].at[shard, :, cols(j)],
                      co_s.at[w, j, idx], co_r.at[w, j, idx], flip(me, 1))

    def co_own(w):
        return remote(srcs[w], alls[w].at[me], co_s.at[w, 0, 7], co_r.at[w, 0, 7], flip(me, 1))

    def ag_send(w, stage):
        for t in range((1, 2, 4)[stage]):
            for j in range(3):
                ag_copy(w, j, stage, t).start()

    def ag_arrive(w, stage):
        for t in range((1, 2, 4)[stage]):
            for j in range(3):
                ag_copy(w, j, stage, t).wait_recv()

    def co_send(w, stage):
        for t in range((1, 2, 4)[stage]):
            for j in range(3):
                co_copy(w, j, (0, 1, 3)[stage] + t).start()

    def co_arrive(w):
        for idx in range(7):
            for j in range(3):
                co_copy(w, j, idx).wait_recv()
        co_own(w).wait_recv()

    ag_send(0, 0)
    ag_send(1, 0)
    co_own(0).start()
    co_own(1).start()

    ld_x.wait()
    st_x = pltpu.make_async_copy(xv, xall.at[me], loc.at[4]); st_x.start()
    logits = dot(xv[...], wr_ref[...]) + br_ref[...]
    eid, sid = eid_ref[...], sid_ref[...]
    experts = lane((T, NDEV))
    pick = [jnp.sum(jnp.where(eid[:, k:k + 1] == experts, logits, 0.0), axis=1, keepdims=True) for k in range(4)]
    top = functools.reduce(jnp.maximum, pick)
    ex = [jnp.exp(v - top) for v in pick]
    den = ex[0] + ex[1] + ex[2] + ex[3]
    gate = [v / den for v in ex]
    code = [jnp.where(sid[:, k:k + 1] >= 0, eid[:, k:k + 1] * C + sid[:, k:k + 1], -1).astype(F32) for k in range(4)]
    ln = lane((T, 128))
    packed = jnp.zeros((T, 128), F32)
    for k in range(4):
        packed = jnp.where(ln == k, code[k], packed)
        packed = jnp.where(ln == 4 + k, gate[k], packed)
    mcol[...] = packed
    meta[me] = packed.T[:8]
    er, ec = sub((256, 256)), lane((256, 256))
    emat[...] = jnp.where(jnp.where(ec < 128, 2 * ec, 2 * (ec - 128) + 1) == er, 1.0, 0.0).astype(BF)
    wd[pl.ds(F, FP - F), :] = jnp.zeros((FP - F, D), BF)
    ld_dy.wait()
    st_dy = pltpu.make_async_copy(dyv, dyall.at[me], loc.at[5]); st_dy.start()

    def meta_copy(m):
        return remote(meta.at[me], meta.at[me], me_s.at[m], me_r.at[m], flip(me, m))

    ag_arrive(0, 0)
    ag_send(0, 1)
    co_send(0, 0)
    for m in range(1, NDEV):
        meta_copy(m).start()
    ag_arrive(1, 0)
    ag_send(1, 1)
    co_send(1, 0)
    ag_arrive(0, 1)
    ag_send(0, 2)
    co_send(0, 1)
    ag_arrive(1, 1)
    ag_send(1, 2)
    co_send(1, 1)
    st_x.wait()
    st_dy.wait()
    for m in range(1, NDEV):
        remote(meta.at[me], meta.at[flip(me, m)], me_s.at[m], me_r.at[m], flip(me, m)).wait_recv()
    ld_gu.wait()
    ld_d.wait()
    ag_arrive(0, 2)
    co_send(0, 2)
    co_arrive(0)

    want = (me * C + sub((C, T))).astype(F32)

    def onehot(s):
        mt = meta[s]
        hit = jnp.zeros((C, T), F32)
        wsum = jnp.zeros((C, T), F32)
        for k in range(4):
            eq = want == mt[k:k + 1]
            hit = jnp.where(eq, 1.0, hit)
            wsum = jnp.where(eq, mt[4 + k:5 + k], wsum)
        return hit.astype(BF), wsum

    def shard_loop(src, body):
        def fetch(s, slot):
            return pltpu.make_async_copy(src.at[s], xs.at[slot], tile_sem.at[slot])
        fetch(0, 0).start()

        def step(s, carry):
            slot = lax.rem(s, 2)

            @pl.when(s + 1 < NDEV)
            def _():
                fetch(s + 1, 1 - slot).start()
            fetch(s, slot).wait()
            body(s, slot)
            return carry
        lax.fori_loop(0, NDEV, step, 0)

    CW = 1024

    def take_x(s, slot):
        hit, _ = onehot(s)
        row = pl.multiple_of(s * C, 16)
        for c in range(D // CW):
            rx[pl.ds(row, C), c * CW:(c + 1) * CW] = dot(hit, xs[slot, :, c * CW:(c + 1) * CW]).astype(BF)

    def take_q(s, slot):
        hit, wsum = onehot(s)
        wrow = jnp.sum(wsum, axis=1, keepdims=True)
        row = pl.multiple_of(s * C, 16)
        for c in range(D // CW):
            got = dot(hit, xs[slot, :, c * CW:(c + 1) * CW])
            rq[pl.ds(row, C), c * CW:(c + 1) * CW] = (wrow * got).astype(BF)

    shard_loop(xall, take_x)
    MB = 256

    def fwd_tile(m, n, width):
        rows = pl.ds(pl.multiple_of(m * MB, MB), MB)
        wcol = pl.multiple_of(n * 256, 256) if not isinstance(n, int) else n * 256
        h = dot(rx[rows, :], wgu[:, pl.ds(wcol, width)])
        gu = jnp.zeros((MB, 256), F32)
        for part in split3(h):
            gu = gu + dot(part, emat[:width, :])
        gu = gu + bgu_ref[n]
        g, u = gu[:, :128], gu[:, 128:]
        gc = jnp.minimum(g, SWIGLU_LIMIT)
        uc = jnp.clip(u, -SWIGLU_LIMIT, SWIGLU_LIMIT)
        act = gc * jax.nn.sigmoid(SWIGLU_ALPHA * gc) * (uc + 1.0)
        acol = pl.multiple_of(n * 128, 128) if not isinstance(n, int) else n * 128
        gs[rows, pl.ds(acol, 128)] = g
        us[rows, pl.ds(acol, 128)] = u
        asc[rows, pl.ds(acol, 128)] = act.astype(BF)

    def bwd_tile(m, n, width):
        rows = pl.ds(pl.multiple_of(m * MB, MB), MB)
        acol = pl.multiple_of(n * 128, 128) if not isinstance(n, int) else n * 128
        wcol = pl.multiple_of(n * 256, 256) if not isinstance(n, int) else n * 256
        da = dot_nt(rq[rows, :], wd[pl.ds(acol, 128), :])
        g, u = gs[rows, pl.ds(acol, 128)], us[rows, pl.ds(acol, 128)]
        gc = jnp.minimum(g, SWIGLU_LIMIT)
        uc = jnp.clip(u, -SWIGLU_LIMIT, SWIGLU_LIMIT)
        sg = jax.nn.sigmoid(SWIGLU_ALPHA * gc)
        glu = gc * sg
        dg = da * (uc + 1.0) * (sg + SWIGLU_ALPHA * glu * (1.0 - sg))
        du = da * glu
        au = jnp.abs(u)
        dg = dg * jnp.where(g < SWIGLU_LIMIT, 1.0, jnp.where(g > SWIGLU_LIMIT, 0.0, 0.5))
        du = du * jnp.where(au < SWIGLU_LIMIT, 1.0, jnp.where(au > SWIGLU_LIMIT, 0.0, 0.5))
        pair = jnp.concatenate([dg.astype(BF), du.astype(BF)], axis=1)
        dh[rows, pl.ds(wcol, width)] = dot_nt(pair, emat[:width, :]).astype(BF)

    def tiles(fn):
        full = F2 // 256

        def row_step(m, carry):
            def step(n, c):
                fn(m, n, 256)
                return c
            lax.fori_loop(0, full, step, 0)
            if F2 % 256:
                fn(m, full, F2 % 256)
            return carry
        lax.fori_loop(0, R // MB, row_step, 0)

    tiles(fwd_tile)
    YW = 256

    def y_step(i, carry):
        m, n = lax.div(i, D // YW), lax.rem(i, D // YW)
        rows = pl.ds(pl.multiple_of(m * MB, MB), MB)
        col = pl.ds(pl.multiple_of(n * YW, YW), YW)
        yv[rows, col] = (dot(asc[rows, :], wd[:, col]) + bd_ref[:, col]).astype(BF)
        return carry
    lax.fori_loop(0, (R // MB) * (D // YW), y_step, 0)

    order = [c * 2 + k for c in CHIP_ORDER for k in (0, 1)]
    order.insert(0, 1)

    def ret_copy(buf, dst, ss, rs, m):
        d = flip(me, m)
        return remote(buf.at[pl.ds(d * C, C)], dst.at[me], ss.at[m], rs.at[m], d)

    for m in order:
        ret_copy(yv, yret, ya_s, ya_r, m).start()
    st = [pltpu.make_async_copy(rx, rx_o, loc.at[6]), pltpu.make_async_copy(asc, a_o, loc.at[7])]
    for s in st:
        s.start()

    ag_arrive(1, 2)
    co_send(1, 2)
    co_arrive(1)
    shard_loop(dyall, take_q)
    tiles(bwd_tile)

    def p_step(i, carry):
        m, n = lax.div(i, D // YW), lax.rem(i, D // YW)
        rows = pl.ds(pl.multiple_of(m * MB, MB), MB)
        off = pl.ds(pl.multiple_of(n * YW, YW), YW)
        pv[rows, off] = dot_nt(dh[rows, :], wgu[off, :]).astype(BF)
        return carry
    lax.fori_loop(0, (R // MB) * (D // YW), p_step, 0)
    early, late = order[:-2], order[-2:]
    for m in early:
        ret_copy(pv, pret, pa_s, pa_r, m).start()
    st += [pltpu.make_async_copy(rq, q_o, loc.at[8]), pltpu.make_async_copy(dh, dh_o, loc.at[9])]
    for s in st[2:]:
        s.start()
    ones = jnp.ones((8, R), BF)

    def bd_step(n, carry):
        col = pl.ds(pl.multiple_of(n * 512, 512), 512)
        dbd_ref[:, col] = dot(ones, rq[:, col])
        return carry
    lax.fori_loop(0, D // 512, bd_step, 0)
    dbgu_ref[...] = dot(ones, dh[...])

    def get_cols():
        pk = mcol[...]
        return [pk[:, k:k + 1] for k in range(4)], [pk[:, 4 + k:5 + k] for k in range(4)]

    def hits(e):
        cd, gt = get_cols()
        pos = (e * C + lane((T, C))).astype(F32)
        return [cd[k] == pos for k in range(4)], gt

    def ret_loop(buf, dst, rs, first, body, carry):
        def fetch(i, slot):
            e = flip(me, i)
            return pltpu.make_async_copy(dst.at[e], xs.at[slot, pl.ds(0, C)], tile_sem.at[slot])

        def arrived(m):
            e = flip(me, m)
            return remote(buf.at[pl.ds(e * C, C)], dst.at[e], ya_s.at[0], rs.at[m], e)
        for m in order:
            arrived(m).wait_recv()
        own = pltpu.make_async_copy(buf.at[pl.ds(me * C, C)], dst.at[me], loc.at[first])
        own.start()
        own.wait()
        fetch(0, 0).start()

        def step(i, c):
            slot = lax.rem(i, 2)

            @pl.when(i + 1 < NDEV)
            def _():
                fetch(i + 1, 1 - slot).start()
            fetch(i, slot).wait()
            return body(flip(me, i), slot, c)
        return lax.fori_loop(0, NDEV, step, carry)

    acc[...] = jnp.zeros((T, D), F32)

    def add_y(e, slot, rs):
        hk, gt = hits(e)
        cw = jnp.zeros((T, C), F32)
        for k in range(4):
            cw = jnp.where(hk[k], gt[k], cw)
        c3 = jnp.concatenate(split3(cw), axis=0)
        for c in range(D // CW):
            cc = slice(c * CW, (c + 1) * CW)
            v = dot(c3, xs[slot, :C, cc])
            acc[:, cc] += v[:T] + v[T:2 * T] + v[2 * T:]
        rm = dot_nt(dyv[...], xs[slot, :C, :])
        return tuple(rs[k] + jnp.sum(jnp.where(hk[k], rm, 0.0), axis=1, keepdims=True) for k in range(4))

    zero = jnp.zeros((T, 1), F32)
    rk = ret_loop(yv, yret, ya_r, 10, add_y, (zero,) * 4)
    out_ref[...] = acc[...].astype(BF)
    _, gt = get_cols()
    mean = gt[0] * rk[0] + gt[1] * rk[1] + gt[2] * rk[2] + gt[3] * rk[3]
    eid = eid_ref[...]
    dl = jnp.zeros((T, 128), F32)
    for k in range(4):
        dl = jnp.where(eid[:, k:k + 1] == ln, gt[k] * (rk[k] - mean), dl)
    dlall[me] = dl.T[:NDEV].astype(BF)
    dlb = dl.astype(BF)[:, :NDEV]
    for c in range(D // CW):
        cc = slice(c * CW, (c + 1) * CW)
        acc[:, cc] = dot_nt(dlb, wr_ref[cc, :])

    def dl_copy(m):
        return remote(dlall.at[me], dlall.at[me], dl_s.at[m], dl_r.at[m], flip(me, m))

    for m in range(1, NDEV):
        dl_copy(m).start()
    for m in late:
        ret_copy(pv, pret, pa_s, pa_r, m).start()

    for m in range(1, NDEV):
        e = flip(me, m)
        remote(dlall.at[me], dlall.at[e], dl_s.at[m], dl_r.at[m], e).wait_recv()
    dwr_ref[...] = jnp.zeros(dwr_ref.shape, F32)
    dbr_ref[...] = jnp.zeros(dbr_ref.shape, F32)

    def add_wr(s, slot):
        dls = dlall[s]
        dbr_ref[...] += dls.astype(F32)
        for c in range(D // CW):
            cc = slice(c * CW, (c + 1) * CW)
            dwr_ref[:, cc] += dot(dls, xs[slot, :, cc])
    shard_loop(xall, add_wr)

    def add_p(e, slot, carry):
        hk, _ = hits(e)
        hit = jnp.zeros((T, C), F32)
        for k in range(4):
            hit = jnp.where(hk[k], 1.0, hit)
        hb = hit.astype(BF)
        for c in range(D // CW):
            cc = slice(c * CW, (c + 1) * CW)
            acc[:, cc] += dot(hb, xs[slot, :C, cc])
        return carry
    ret_loop(pv, pret, pa_r, 11, add_p, 0)
    dx_ref[...] = acc[...].astype(BF)

    for w in range(2):
        co_own(w).wait_send()
        for j in range(3):
            for stage in range(3):
                for t in range((1, 2, 4)[stage]):
                    ag_copy(w, j, stage, t).wait_send()
            for idx in range(7):
                co_copy(w, j, idx).wait_send()
    for m in range(1, NDEV):
        meta_copy(m).wait_send()
        dl_copy(m).wait_send()
        ret_copy(yv, yret, ya_s, ya_r, m).wait_send()
        ret_copy(pv, pret, pa_s, pa_r, m).wait_send()
    for s in st:
        s.wait()


def solution(mesh):
    def local_block(hidden, grad_out, w_router, b_router, expert_ids, slot_ids, w_gate_up, b_gate_up, w_down, b_down):
        T, D = hidden.shape
        F = w_down.shape[1]
        C = (3 * T * 4 + 2 * NDEV - 1) // (2 * NDEV)
        R = NDEV * C
        NT = -(-F // 128)
        FP = NT * 128
        bias = jnp.pad(b_gate_up.reshape(F, 2), ((0, FP - F), (0, 0))).reshape(NT, 128, 2)
        bias = bias.transpose(0, 2, 1).reshape(NT, 1, 256)
        S = jax.ShapeDtypeStruct
        vm, hb = pl.BlockSpec(memory_space=pltpu.VMEM), pl.BlockSpec(memory_space=pl.ANY)
        outs = [S((T, D), BF), S((T, D), BF), S((NDEV, D), F32), S((NDEV, T), F32), S((8, D), F32), S((8, 2 * F), F32),
                S((R, D), BF), S((R, D), BF), S((R, FP), BF), S((R, 2 * F), BF),
                S((NDEV, T, D), BF), S((NDEV, T, D), BF), S((NDEV, C, D), BF), S((NDEV, C, D), BF)]
        V, dma = pltpu.VMEM, pltpu.SemaphoreType.DMA
        scratch = [V((D, 2 * F), BF), V((FP, D), BF), V((R, D), BF), V((R, D), BF), V((R, FP), F32), V((R, FP), F32),
                   V((R, FP), BF), V((R, 2 * F), BF), V((R, D), BF), V((R, D), BF), V((2, T, D), BF), V((T, D), BF),
                   V((T, D), BF), V((T, D), F32), V((NDEV, 8, T), F32), V((NDEV, NDEV, T), BF), V((T, 128), F32),
                   V((256, 256), BF),
                   dma((2, 3, 7)), dma((2, 3, 7)), dma((2, 3, 8)), dma((2, 3, 8)),
                   dma((16,)), dma((16,)), dma((16,)), dma((16,)), dma((16,)), dma((16,)), dma((16,)), dma((16,)),
                   dma((12,)), dma((2,))]
        res = pl.pallas_call(
            functools.partial(block_kernel, (T, D, F, C)),
            out_shape=outs,
            in_specs=[hb, hb, vm, vm, vm, vm, hb, vm, hb, vm],
            out_specs=[vm, vm, vm, vm, vm, vm] + [hb] * 8,
            scratch_shapes=scratch,
            compiler_params=pltpu.CompilerParams(collective_id=0, has_side_effects=True, vmem_limit_bytes=67043328),
            name="moe_block",
        )(hidden, grad_out, w_router, b_router.reshape(1, NDEV), expert_ids, slot_ids,
          w_gate_up[0], bias, w_down[0], b_down)
        out, dx, dwr, dbr, dbd, dbgu, rx, q, a, dh = res[:10]
        grad_w_down = jnp.einsum('rf,rd->fd', a[:, :F], q, preferred_element_type=F32)[None]
        grad_w_gate_up = jnp.einsum('rd,rf->df', rx, dh, preferred_element_type=F32)[None]
        return (out, dx, dwr.T, jnp.sum(dbr, axis=1), grad_w_gate_up, dbgu[:1], grad_w_down, dbd[:1])

    tok = P('ep', None)
    ex3, ex2 = P('ep', None, None), P('ep', None)
    in_specs = (tok, tok, P(None, None), P(None), tok, tok, ex3, ex2, ex3, ex2)
    out_specs = (tok, tok, P(None, None), P(None), ex3, ex2, ex3, ex2)
    return jax.shard_map(local_block, mesh=mesh, in_specs=in_specs, out_specs=out_specs, check_vma=False)
```

```python
import functools

import jax
import jax.numpy as jnp
from jax import lax
from jax.experimental import pallas as pl
from jax.experimental.pallas import tpu as pltpu
from jax.sharding import PartitionSpec as P

SWIGLU_LIMIT = 7.0
SWIGLU_ALPHA = 1.702
MESH_ID = pl.DeviceIdType.MESH
BF = jnp.bfloat16
F32 = jnp.float32

DIMS = (2, 4, 8)
CHIP_ORDER = (3, 4, 5, 2, 6, 1, 7)
NDEV = 16


def flip(me, mask):
    out = 0
    for b in (1, 2, 4, 8):
        bit = lax.rem(lax.div(me, b), 2)
        if isinstance(mask, int):
            if mask & b:
                bit = 1 - bit
        else:
            bit = lax.rem(bit + lax.rem(lax.div(mask, b), 2), 2)
        out = out + b * bit
    return out


def split3(v):
    hi = v.astype(BF)
    rest = v - hi.astype(F32)
    mid = rest.astype(BF)
    low = (rest - mid.astype(F32)).astype(BF)
    return hi, mid, low


def dot(a, b):
    return jnp.dot(a, b, preferred_element_type=F32)


def dot_nt(a, b):
    return lax.dot_general(a, b, (((1,), (1,)), ((), ())), preferred_element_type=F32)


def remote(src, dst, ssem, rsem, dev):
    return pltpu.make_async_remote_copy(src_ref=src, dst_ref=dst, send_sem=ssem, recv_sem=rsem,
                                        device_id=(dev,), device_id_type=MESH_ID)


def block_kernel(cfg, *refs):
    T, D, F, C = cfg
    F2 = 2 * F
    R = NDEV * C
    NT = -(-F // 128)
    FP = NT * 128
    (x_ref, dy_ref, wr_ref, br_ref, eid_ref, sid_ref, wgu_ref, bgu_ref, wd_ref, bd_ref,
     out_ref, dx_ref, dwr_ref, dbr_ref, dbd_ref, dbgu_ref, rx_o, q_o, a_o, dh_o,
     xall, dyall, yret, pret,
     wgu, wd, rx, rq, gs, us, asc, dh, yv, pv, xs, xv, dyv, acc, meta, dlall, mcol, emat, wpart,
     ag_s, ag_r, co_s, co_r, lf_s, lf_r, ya_s, ya_r, pa_s, pa_r, me_s, me_r, dl_s, dl_r, wr_s, wr_r,
     loc, tile_sem) = refs
    me = lax.axis_index("ep")
    core = lax.rem(me, 2)
    lane = lambda shape: lax.broadcasted_iota(jnp.int32, shape, 1)
    sub = lambda shape: lax.broadcasted_iota(jnp.int32, shape, 0)

    ld_x = pltpu.make_async_copy(x_ref, xv, loc.at[0]); ld_x.start()
    ld_dy = pltpu.make_async_copy(dy_ref, dyv, loc.at[1]); ld_dy.start()
    ld_gu = pltpu.make_async_copy(wgu_ref, wgu, loc.at[2]); ld_gu.start()
    ld_d = pltpu.make_async_copy(wd_ref, wd.at[pl.ds(0, F)], loc.at[3]); ld_d.start()

    bar = pltpu.get_barrier_semaphore()
    for m in range(1, NDEV):
        pl.semaphore_signal(bar, inc=1, device_id=(flip(me, m),), device_id_type=MESH_ID)
    pl.semaphore_wait(bar, NDEV - 1)

    cuts = [0, 11 * D // 32, 22 * D // 32, D]
    srcs, alls, rows_of, stage_of = (x_ref, dy_ref), (xall, dyall), (rx, rq), (yv, pv)
    local = (xv, dyv)
    dims = [(DIMS[j], DIMS[(j + 1) % 3], DIMS[(j + 2) % 3]) for j in range(3)]
    plane = [(0, a, b, a ^ b) for a, b, _ in dims]

    def cols(j):
        return pl.ds(cuts[j], cuts[j + 1] - cuts[j])

    def ag_copy(w, j, idx):
        a, b, _ = dims[j]
        off = (0, 0, a)[idx]
        shard = flip(me, off)
        src = srcs[w].at[:, cols(j)] if off == 0 else alls[w].at[shard, :, cols(j)]
        return remote(src, alls[w].at[shard, :, cols(j)], ag_s.at[w, j, idx], ag_r.at[w, j, idx],
                      flip(me, (a, b, b)[idx]))

    def co_copy(w, j, t):
        shard = flip(me, plane[j][t])
        src = srcs[w].at[:, cols(j)] if t == 0 else alls[w].at[shard, :, cols(j)]
        return remote(src, alls[w].at[shard, :, cols(j)], co_s.at[w, j, t], co_r.at[w, j, t], flip(me, 1))

    def lf_copy(w, j, t, k):
        shard = flip(me, plane[j][t])
        there = lax.div(flip(me, dims[j][2]), 2) * 2
        return remote(stage_of[w].at[pl.ds(t * 2 * C + k * C, C), cols(j)],
                      rows_of[w].at[pl.ds(pl.multiple_of(shard * C, 16), C), cols(j)],
                      lf_s.at[w, j, t, k], lf_r.at[w, j, t, core], there + k)

    def lf_arrive(w):
        for t in range(4):
            for j in range(3):
                there = lax.div(flip(me, dims[j][2]), 2) * 2
                for k in range(2):
                    shard = flip(there + k, plane[j][t])
                    remote(stage_of[w].at[pl.ds(t * 2 * C + k * C, C), cols(j)],
                           rows_of[w].at[pl.ds(pl.multiple_of(shard * C, 16), C), cols(j)],
                           lf_s.at[w, j, t, k], lf_r.at[w, j, t, k], there + k).wait_recv()

    def compact(w, j, t, s, src, leaf):
        mt = meta[s]
        M = 3 * C if leaf else C
        pos = sub((M, T))
        want = me * C + pos
        if leaf:
            there = lax.div(flip(me, dims[j][2]), 2) * 2
            want = jnp.where(pos < C, want, there * C + pos - C)
        want = want.astype(F32)
        hit = jnp.zeros((M, T), F32)
        wsum = jnp.zeros((M, T), F32)
        for k in range(4):
            eq = want == mt[k:k + 1]
            hit = jnp.where(eq, 1.0, hit)
            if w:
                wsum = jnp.where(eq, mt[4 + k:5 + k], wsum)
        hb = hit.astype(BF)
        wrow = jnp.sum(wsum, axis=1, keepdims=True)
        row = pl.multiple_of(s * C, 16)
        c0 = cuts[j]
        while c0 < cuts[j + 1]:
            c1 = min(c0 + 512, cuts[j + 1])
            got = dot(hb, src[:, c0:c1])
            if w:
                got = wrow * got
            got = got.astype(BF)
            rows_of[w][pl.ds(row, C), c0:c1] = got[:C]
            if leaf:
                stage_of[w][t * 2 * C:(t + 1) * 2 * C, c0:c1] = got[C:]
            c0 = c1

    def load_part(w, j, s, slot):
        return pltpu.make_async_copy(alls[w].at[s, :, cols(j)], xs.at[slot, :, cols(j)], tile_sem.at[slot, j])

    def issue_own(w):
        for idx in (0, 1):
            for j in range(3):
                ag_copy(w, j, idx).start()
        for j in range(3):
            co_copy(w, j, 0).start()

    def issue_leaf_own(w):
        for j in range(3):
            compact(w, j, 0, me, local[w], True)
            for k in range(2):
                lf_copy(w, j, 0, k).start()

    def relay(w, idx):
        slot = idx % 2
        t = idx + 1
        for j in range(3):
            ag_copy_in(w, j, idx).wait_recv()
            if idx == 0:
                ag_copy(w, j, 2).start()
            co_copy(w, j, t).start()
            load_part(w, j, flip(me, plane[j][t]), slot).start()
        for j in range(3):
            s = flip(me, plane[j][t])
            load_part(w, j, s, slot).wait()
            compact(w, j, t, s, xs.at[slot], True)
            for k in range(2):
                lf_copy(w, j, t, k).start()

    def ag_copy_in(w, j, idx):
        shard = flip(me, plane[j][idx + 1])
        a, b, _ = dims[j]
        return remote(srcs[w].at[:, cols(j)], alls[w].at[shard, :, cols(j)], ag_s.at[w, j, idx], ag_r.at[w, j, idx],
                      flip(me, (a, b, b)[idx]))

    def siblings(w):
        other = flip(me, 1)

        def begin(t):
            for j in range(3):
                shard = flip(other, plane[j][t])
                remote(srcs[w].at[:, cols(j)], alls[w].at[shard, :, cols(j)], co_s.at[w, j, t], co_r.at[w, j, t],
                       other).wait_recv()
                load_part(w, j, shard, t % 2).start()
        begin(0)
        for t in range(4):
            if t < 3:
                begin(t + 1)
            for j in range(3):
                shard = flip(other, plane[j][t])
                load_part(w, j, shard, t % 2).wait()
                compact(w, j, t, shard, xs.at[t % 2], False)

    issue_own(0)

    ld_x.wait()
    st_x = pltpu.make_async_copy(xv, xall.at[me], loc.at[4]); st_x.start()
    logits = dot_nt(wr_ref[...], xv[...]) + br_ref[...]
    eid, sid = eid_ref[...], sid_ref[...]
    experts = sub((NDEV, T))
    pick = [jnp.sum(jnp.where(eid[k:k + 1] == experts, logits, 0.0), axis=0, keepdims=True) for k in range(4)]
    top = functools.reduce(jnp.maximum, pick)
    ex = [jnp.exp(v - top) for v in pick]
    den = ex[0] + ex[1] + ex[2] + ex[3]
    sb = sub((T, T))
    packed = jnp.zeros((T, T), F32)
    for k in range(4):
        code = jnp.where(sid[k:k + 1] >= 0, eid[k:k + 1] * C + sid[k:k + 1], -1).astype(F32)
        packed = jnp.where(sb == k, code, packed)
        packed = jnp.where(sb == 4 + k, ex[k] / den, packed)
        packed = jnp.where(sb == 8 + k, eid[k:k + 1].astype(F32), packed)
    mcol[...] = packed.T
    meta[me] = packed[:8]
    er, ec = sub((256, 256)), lane((256, 256))
    emat[...] = jnp.where(jnp.where(ec < 128, 2 * ec, 2 * (ec - 128) + 1) == er, 1.0, 0.0).astype(BF)

    def meta_copy(m):
        return remote(meta.at[me], meta.at[me], me_s.at[m], me_r.at[m], flip(me, m))

    compact(0, 0, 0, me, local[0], True)
    for m in range(1, NDEV):
        meta_copy(m).start()
    issue_leaf_own(0)
    wd[pl.ds(F, FP - F), :] = jnp.zeros((FP - F, D), BF)
    for m in range(1, NDEV):
        remote(meta.at[me], meta.at[flip(me, m)], me_s.at[m], me_r.at[m], flip(me, m)).wait_recv()
    relay(0, 0)
    relay(0, 1)
    relay(0, 2)
    issue_own(1)
    ld_dy.wait()
    issue_leaf_own(1)
    siblings(0)
    st_x.wait()
    ld_gu.wait()
    ld_d.wait()
    lf_arrive(0)

    MB = 256

    def fwd_tile(m, n, width):
        rows = pl.ds(pl.multiple_of(m * MB, MB), MB)
        wrow = pl.multiple_of(n * 256, 256) if not isinstance(n, int) else n * 256
        h = dot_nt(rx[rows, :], wgu[pl.ds(wrow, width), :])
        gu = jnp.zeros((MB, 256), F32)
        for part in split3(h):
            gu = gu + dot(part, emat[:width, :])
        gu = gu + bgu_ref[n]
        g, u = gu[:, :128], gu[:, 128:]
        gc = jnp.minimum(g, SWIGLU_LIMIT)
        uc = jnp.clip(u, -SWIGLU_LIMIT, SWIGLU_LIMIT)
        act = gc * jax.nn.sigmoid(SWIGLU_ALPHA * gc) * (uc + 1.0)
        acol = pl.multiple_of(n * 128, 128) if not isinstance(n, int) else n * 128
        gs[rows, pl.ds(acol, 128)] = g
        us[rows, pl.ds(acol, 128)] = u
        asc[rows, pl.ds(acol, 128)] = act.astype(BF)

    def bwd_tile(m, n, width):
        rows = pl.ds(pl.multiple_of(m * MB, MB), MB)
        acol = pl.multiple_of(n * 128, 128) if not isinstance(n, int) else n * 128
        wcol = pl.multiple_of(n * 256, 256) if not isinstance(n, int) else n * 256
        da = dot_nt(rq[rows, :], wd[pl.ds(acol, 128), :])
        g, u = gs[rows, pl.ds(acol, 128)], us[rows, pl.ds(acol, 128)]
        gc = jnp.minimum(g, SWIGLU_LIMIT)
        uc = jnp.clip(u, -SWIGLU_LIMIT, SWIGLU_LIMIT)
        sg = jax.nn.sigmoid(SWIGLU_ALPHA * gc)
        glu = gc * sg
        dg = da * (uc + 1.0) * (sg + SWIGLU_ALPHA * glu * (1.0 - sg))
        du = da * glu
        au = jnp.abs(u)
        dg = dg * jnp.where(g < SWIGLU_LIMIT, 1.0, jnp.where(g > SWIGLU_LIMIT, 0.0, 0.5))
        du = du * jnp.where(au < SWIGLU_LIMIT, 1.0, jnp.where(au > SWIGLU_LIMIT, 0.0, 0.5))
        pair = jnp.concatenate([dg.astype(BF), du.astype(BF)], axis=1)
        dh[rows, pl.ds(wcol, width)] = dot_nt(pair, emat[:width, :]).astype(BF)

    def tiles(fn, lo, hi):
        full = F2 // 256

        def row_step(m, carry):
            def step(n, c):
                fn(m, n, 256)
                return c
            lax.fori_loop(0, full, step, 0)
            if F2 % 256:
                fn(m, full, F2 % 256)
            return carry
        lax.fori_loop(lo, hi, row_step, 0)

    YW = 256
    NY = D // YW

    def y_step(i, carry):
        m, n = lax.div(i, NY), lax.rem(i, NY)
        rows = pl.ds(pl.multiple_of(m * MB, MB), MB)
        col = pl.ds(pl.multiple_of(n * YW, YW), YW)
        yv[rows, col] = (dot(asc[rows, :], wd[:, col]) + bd_ref[:, col]).astype(BF)
        return carry

    tiles(fwd_tile, 0, 1)
    relay(1, 0)
    relay(1, 1)
    tiles(fwd_tile, 1, R // MB)
    for t in range(4):
        for j in range(3):
            for k in range(2):
                lf_copy(0, j, t, k).wait_send()
    lax.fori_loop(0, NY, y_step, 0)
    relay(1, 2)
    lax.fori_loop(NY, (R // MB) * NY, y_step, 0)

    order = [c * 2 + k for c in CHIP_ORDER for k in (0, 1)]
    order.insert(0, 1)

    def ret_copy(buf, dst, ss, rs, m):
        d = flip(me, m)
        return remote(buf.at[pl.ds(pl.multiple_of(d * C, 16), C)], dst.at[me], ss.at[m], rs.at[m], d)

    for m in order:
        ret_copy(yv, yret, ya_s, ya_r, m).start()
    st = [pltpu.make_async_copy(rx, rx_o, loc.at[6]), pltpu.make_async_copy(asc, a_o, loc.at[7])]
    for s in st:
        s.start()

    siblings(1)
    lf_arrive(1)
    tiles(bwd_tile, 0, R // MB)
    for t in range(4):
        for j in range(3):
            for k in range(2):
                lf_copy(1, j, t, k).wait_send()

    def p_step(i, carry):
        m, n = lax.div(i, NY), lax.rem(i, NY)
        rows = pl.ds(pl.multiple_of(m * MB, MB), MB)
        col = pl.ds(pl.multiple_of(n * YW, YW), YW)
        pv[rows, col] = dot(dh[rows, :], wgu[:, col]).astype(BF)
        return carry
    lax.fori_loop(0, (R // MB) * NY, p_step, 0)
    first, second, last = order[:5], order[5:13], order[13:]
    for m in first:
        ret_copy(pv, pret, pa_s, pa_r, m).start()
    st += [pltpu.make_async_copy(rq, q_o, loc.at[8]), pltpu.make_async_copy(dh, dh_o, loc.at[9])]
    for s in st[2:]:
        s.start()
    ones = jnp.ones((8, R), BF)

    def bd_step(n, carry):
        col = pl.ds(pl.multiple_of(n * 512, 512), 512)
        dbd_ref[:, col] = dot(ones, rq[:, col])[:1]
        return carry
    lax.fori_loop(0, D // 512, bd_step, 0)
    dbgu_ref[...] = dot(ones, dh[...])[:1]

    CW = 1024
    ln = lane((T, 128))

    def get_cols(base):
        pk = mcol[...]
        return [pk[:, base + k:base + k + 1] for k in range(4)]

    def hits(e):
        cd = get_cols(0)
        pos = (e * C + lane((T, C))).astype(F32)
        return [cd[k] == pos for k in range(4)]

    def ret_loop(buf, dst, ss, rs, first, body, carry):
        own = pltpu.make_async_copy(buf.at[pl.ds(pl.multiple_of(me * C, 16), C)], dst.at[me], loc.at[first])
        own.start()
        own.wait()

        def step(i, c):
            e = flip(me, i)

            @pl.when(i > 0)
            def _():
                remote(buf.at[pl.ds(0, C)], dst.at[e], ss.at[i], rs.at[i], e).wait_recv()
            get = pltpu.make_async_copy(dst.at[e], xs.at[0, pl.ds(0, C)], loc.at[first])
            get.start()
            get.wait()
            return body(e, c)
        return lax.fori_loop(0, NDEV, step, carry)

    acc[...] = jnp.zeros((T, D), F32)

    def add_y(e, rs):
        hk, gt = hits(e), get_cols(4)
        cw = jnp.zeros((T, C), F32)
        for k in range(4):
            cw = jnp.where(hk[k], gt[k], cw)
        c3 = jnp.concatenate(split3(cw), axis=0)
        for c in range(D // CW):
            cc = slice(c * CW, (c + 1) * CW)
            v = dot(c3, xs[0, :C, cc])
            acc[:, cc] += v[:T] + v[T:2 * T] + v[2 * T:]
        rm = dot_nt(dyv[...], xs[0, :C, :])
        return tuple(rs[k] + jnp.sum(jnp.where(hk[k], rm, 0.0), axis=1, keepdims=True) for k in range(4))

    zero = jnp.zeros((T, 1), F32)
    rk = ret_loop(yv, yret, ya_s, ya_r, 10, add_y, (zero,) * 4)
    gt, ei = get_cols(4), get_cols(8)
    mean = gt[0] * rk[0] + gt[1] * rk[1] + gt[2] * rk[2] + gt[3] * rk[3]
    dl = jnp.zeros((T, 128), F32)
    for k in range(4):
        dl = jnp.where(ei[k] == ln.astype(F32), gt[k] * (rk[k] - mean), dl)
    dlall[me] = dl.T[:NDEV].astype(BF)
    out_ref[...] = acc[...].astype(BF)
    dlb = dl.astype(BF)[:, :NDEV]

    def dl_copy(m):
        return remote(dlall.at[me], dlall.at[me], dl_s.at[m], dl_r.at[m], flip(me, m))

    for m in range(1, NDEV):
        dl_copy(m).start()
    for m in second:
        ret_copy(pv, pret, pa_s, pa_r, m).start()
    for c in range(D // CW):
        cc = slice(c * CW, (c + 1) * CW)
        acc[:, cc] = dot(dlb, wr_ref[:, cc])

    for m in range(1, NDEV):
        e = flip(me, m)
        remote(dlall.at[me], dlall.at[e], dl_s.at[m], dl_r.at[m], e).wait_recv()
    dwr_ref[...] = jnp.zeros(dwr_ref.shape, F32)

    def wr_begin(i):
        for j in range(3):
            load_part(0, j, flip(flip(me, i % 2), plane[j][i // 2]), i % 2).start()
    wr_begin(0)
    for i in range(8):
        if i < 7:
            wr_begin(i + 1)
        for j in range(3):
            s = flip(flip(me, i % 2), plane[j][i // 2])
            load_part(0, j, s, i % 2).wait()
            dwr_ref[:, cuts[j]:cuts[j + 1]] += dot(dlall[s], xs[i % 2, :, cuts[j]:cuts[j + 1]])

    def wr_copy(j):
        return remote(dwr_ref.at[:, cols(j)], wpart.at[:, cols(j)], wr_s.at[j], wr_r.at[j], flip(me, dims[j][2]))

    dbr = jnp.zeros((8, NDEV), F32)
    for s in range(NDEV):
        dbr = dbr + dot_nt(jnp.ones((8, T), BF), dlall[s])
    dbr_ref[...] = dbr[:1]
    for j in range(3):
        wr_copy(j).start()
    for m in last:
        ret_copy(pv, pret, pa_s, pa_r, m).start()

    def add_p(e, carry):
        hk = hits(e)
        hit = jnp.zeros((T, C), F32)
        for k in range(4):
            hit = jnp.where(hk[k], 1.0, hit)
        hb = hit.astype(BF)
        for c in range(D // CW):
            cc = slice(c * CW, (c + 1) * CW)
            acc[:, cc] += dot(hb, xs[0, :C, cc])
        return carry
    ret_loop(pv, pret, pa_s, pa_r, 11, add_p, 0)
    dx_ref[...] = acc[...].astype(BF)
    for j in range(3):
        wr_copy(j).wait()
    dwr_ref[...] = dwr_ref[...] + wpart[...]

    for w in range(2):
        for j in range(3):
            for idx in range(3):
                ag_copy(w, j, idx).wait_send()
            for t in range(4):
                co_copy(w, j, t).wait_send()
    for m in range(1, NDEV):
        meta_copy(m).wait_send()
        dl_copy(m).wait_send()
        ret_copy(yv, yret, ya_s, ya_r, m).wait_send()
        ret_copy(pv, pret, pa_s, pa_r, m).wait_send()
    for s in st:
        s.wait()


def solution(mesh):
    def local_block(hidden, grad_out, w_router, b_router, expert_ids, slot_ids, w_gate_up, b_gate_up, w_down, b_down):
        T, D = hidden.shape
        F = w_down.shape[1]
        C = (3 * T * 4 + 2 * NDEV - 1) // (2 * NDEV)
        R = NDEV * C
        NT = -(-F // 128)
        FP = NT * 128
        bias = jnp.pad(b_gate_up.reshape(F, 2), ((0, FP - F), (0, 0))).reshape(NT, 128, 2)
        bias = bias.transpose(0, 2, 1).reshape(NT, 1, 256)
        S = jax.ShapeDtypeStruct
        vm, hb = pl.BlockSpec(memory_space=pltpu.VMEM), pl.BlockSpec(memory_space=pl.ANY)
        outs = [S((T, D), BF), S((T, D), BF), S((NDEV, D), F32), S((1, NDEV), F32), S((1, D), F32), S((1, 2 * F), F32),
                S((R, D), BF), S((R, D), BF), S((R, FP), BF), S((R, 2 * F), BF),
                S((NDEV, T, D), BF), S((NDEV, T, D), BF), S((NDEV, C, D), BF), S((NDEV, C, D), BF)]
        V, dma = pltpu.VMEM, pltpu.SemaphoreType.DMA
        scratch = [V((2 * F, D), BF), V((FP, D), BF), V((R, D), BF), V((R, D), BF), V((R, FP), F32), V((R, FP), F32),
                   V((R, FP), BF), V((R, 2 * F), BF), V((R, D), BF), V((R, D), BF), V((2, T, D), BF), V((T, D), BF),
                   V((T, D), BF), V((T, D), F32), V((NDEV, 8, T), F32), V((NDEV, NDEV, T), BF), V((T, 128), F32),
                   V((256, 256), BF), V((NDEV, D), F32),
                   dma((2, 3, 3)), dma((2, 3, 3)), dma((2, 3, 4)), dma((2, 3, 4)), dma((2, 3, 4, 2)), dma((2, 3, 4, 2)),
                   dma((16,)), dma((16,)), dma((16,)), dma((16,)), dma((16,)), dma((16,)), dma((16,)), dma((16,)),
                   dma((3,)), dma((3,)), dma((12,)), dma((2, 3))]
        res = pl.pallas_call(
            functools.partial(block_kernel, (T, D, F, C)),
            out_shape=outs,
            in_specs=[hb, hb, vm, vm, vm, vm, hb, vm, hb, vm],
            out_specs=[vm, vm, vm, vm, vm, vm] + [hb] * 8,
            scratch_shapes=scratch,
            compiler_params=pltpu.CompilerParams(collective_id=0, has_side_effects=True, vmem_limit_bytes=67043328),
            name="moe_block",
        )(hidden, grad_out, w_router.T, b_router.reshape(NDEV, 1), expert_ids.T, slot_ids.T,
          w_gate_up[0].T, bias, w_down[0], b_down)
        out, dx, dwr, dbr, dbd, dbgu, rx, q, a, dh = res[:10]
        grad_w_down = jnp.einsum('rf,rd->fd', a[:, :F], q, preferred_element_type=F32)[None]
        grad_w_gate_up = jnp.einsum('rd,rf->df', rx, dh, preferred_element_type=F32)[None]
        return (out, dx, dwr.T, dbr[0], grad_w_gate_up, dbgu, grad_w_down, dbd)

    tok = P('ep', None)
    ex3, ex2 = P('ep', None, None), P('ep', None)
    in_specs = (tok, tok, P(None, None), P(None), tok, tok, ex3, ex2, ex3, ex2)
    out_specs = (tok, tok, P(None, None), P(None), ex3, ex2, ex3, ex2)
    return jax.shard_map(local_block, mesh=mesh, in_specs=in_specs, out_specs=out_specs, check_vma=False)
```
